32 devices in a mesh: qrow: 8 (over y, x, core), kcol: 4 (over z).
Axes of the slice: x: 2, y: 2, z: 4, core: 2. Of those that a mesh axis runs over, the one named last changes fastest.
Arguments:
- query_states: bfloat16 [32768, 512], P(('qrow', 'kcol')), may hold values from -8 to 8
- key_states: bfloat16 [32768, 512], P(('kcol', 'qrow')), may hold values from -8 to 8
- value_states: bfloat16 [32768, 512], P(('kcol', 'qrow')), may hold values from -6 to 6
- saved_output: bfloat16 [32768, 512], P(('qrow', 'kcol')), may hold values from -0.59765625 to 0.59765625
- output_grad: bfloat16 [32768, 512], P(('qrow', 'kcol')), may hold values from -6 to 6
- normalizer: float32 [32768, 4], P(('qrow', 'kcol')), as said below
- doc_lengths: int32 [8], replicated, may hold values from 1 to 8192, as said below
Outputs:
- query_grad: bfloat16 [32768, 512], P(('qrow', 'kcol'))
- key_grad: bfloat16 [32768, 512], P(('kcol', 'qrow'))
- value_grad: bfloat16 [32768, 512], P(('kcol', 'qrow'))
The draws below stay inside these ranges and needn't reach their ends.
Inputs may be any that keep to these rules, and one draw needn't show every extreme that they name: `doc_lengths`: the 8 lengths sum to 32768; exactly one of them equals 8192, every other one is smaller. normalizer[p, h] is the logarithm of the sum of exp(scores[h, p, t]) over the t that allowed admits, computed in float32 from query_states, key_states and doc_lengths.
All inputs are finite; a program needn't handle non-finite values.
Results may differ from the reference program's by a relative error of at most 0.005.
Values may be sent and summed in bfloat16 or wider, within the bound.
A program may use at most 704 MiB of HBM per device.

```python
import jax
import jax.numpy as jnp
from jax import lax

HEAD_DIM = 128
KV_HEADS = 4
GROUP = 1
TOK = 32768
DOCS = 8
MOST = 8192


def make_queries(key):
    sample = jnp.clip(jax.random.normal(jax.random.fold_in(key, 101), (TOK, KV_HEADS * GROUP * HEAD_DIM), jnp.float32), -4.0, 4.0)
    return sample.astype(jnp.bfloat16)


def make_keys(key):
    sample = jnp.clip(jax.random.normal(jax.random.fold_in(key, 201), (TOK, KV_HEADS * HEAD_DIM), jnp.float32), -4.0, 4.0)
    return sample.astype(jnp.bfloat16)


def make_lengths(key):
    weights = jax.random.randint(jax.random.fold_in(key, 301), (DOCS - 1,), 2, 4).astype(jnp.int32)
    remaining = TOK - MOST - (DOCS - 1)
    others = 1 + remaining * weights // jnp.sum(weights)
    leftover = TOK - MOST - jnp.sum(others)
    others = others + (jnp.arange(DOCS - 1, dtype=jnp.int32) < leftover).astype(jnp.int32)
    longest_at = jax.random.randint(jax.random.fold_in(key, 302), (), 0, DOCS).astype(jnp.int32)
    places = jnp.arange(DOCS, dtype=jnp.int32)
    source = jnp.clip(places - (places > longest_at).astype(jnp.int32), 0, DOCS - 2)
    return jnp.where(places == longest_at, MOST, others[source]).astype(jnp.int32)


def draw_query_states(key, part):
    return make_queries(key)


def draw_key_states(key, part):
    return make_keys(key)


def draw_doc_lengths(key, part):
    return make_lengths(key)


def draw_normalizer(key, part):
    scaling = HEAD_DIM ** (-0.5)
    queries = make_queries(key).astype(jnp.float32).reshape(TOK, KV_HEADS, GROUP, HEAD_DIM).transpose(1, 0, 2, 3)
    keys_all = make_keys(key).astype(jnp.float32).reshape(TOK, KV_HEADS, HEAD_DIM).transpose(1, 0, 2)
    lengths = make_lengths(key)
    positions = jnp.arange(TOK, dtype=jnp.int32)
    doc_ends = jnp.cumsum(lengths)
    documents = jnp.sum((positions[:, None] >= doc_ends[None, :]).astype(jnp.int32), axis=1)
    block_rows = 512 if TOK % 512 == 0 else TOK
    block_count = TOK // block_rows
    window = min(block_rows + MOST, TOK)

    def per_head(operands):
        query_head, key_head = operands

        def per_block(block_index):
            start_row = block_index * block_rows
            key_start = jnp.clip(start_row - MOST, 0, TOK - window).astype(jnp.int32)
            query_rows = lax.dynamic_slice_in_dim(query_head, start_row, block_rows, 0)
            key_rows = lax.dynamic_slice_in_dim(key_head, key_start, window, 0)
            key_pos = lax.dynamic_slice_in_dim(positions, key_start, window, 0)
            key_doc = lax.dynamic_slice_in_dim(documents, key_start, window, 0)
            query_pos = start_row + jnp.arange(block_rows, dtype=jnp.int32)
            query_doc = lax.dynamic_slice_in_dim(documents, start_row, block_rows, 0)
            allowed = (key_pos[None, :] <= query_pos[:, None]) & (key_doc[None, :] == query_doc[:, None])
            scores = jnp.einsum('qgd,kd->qgk', query_rows, key_rows) * scaling
            masked = jnp.where(allowed[:, None, :], scores, -1e+30)
            highest = jnp.max(masked, axis=2, keepdims=True)
            totals = jnp.sum(jnp.where(allowed[:, None, :], jnp.exp(masked - highest), 0.0), axis=2)
            return highest[:, :, 0] + jnp.log(totals)
        return lax.map(per_block, jnp.arange(block_count, dtype=jnp.int32)).reshape(TOK, GROUP)
    result = lax.map(per_head, (queries, keys_all))
    return result.transpose(1, 0, 2).reshape(TOK, KV_HEADS * GROUP).astype(jnp.float32)


def level_of(stream_key, shape, split, smallest, largest):
    def one(position, parts):
        draws = jax.random.uniform(jax.random.fold_in(jax.random.fold_in(stream_key, 6), position), (parts,), jnp.float32, smallest / len(split), largest / len(split))
        return jnp.repeat(jnp.exp(draws), shape[position] // parts).reshape((-1,) + (1,) * (len(shape) - position - 1))

    factor_of = one(*split[0])
    for cut in split[1:]:
        factor_of = factor_of * one(*cut)
    return factor_of


def gaussian(key, dims, deviation, most, shards=(), kind=jnp.bfloat16):
    loudness = level_of(key, dims, shards, -0.22, 0.18) if shards else 1.0
    array = jax.random.normal(key, dims, jnp.float32) * deviation * loudness
    return jnp.minimum(jnp.maximum(array, -most), most).astype(kind)


def setup_inputs(seed: int = 0) -> dict:
    arg_keys = jax.random.split(jax.random.key(seed), 8)
    query_states = draw_query_states(jax.random.fold_in(arg_keys[7], 71), 0)
    key_states = draw_key_states(jax.random.fold_in(arg_keys[7], 71), 0)
    value_states = gaussian(arg_keys[2], (TOK, KV_HEADS * HEAD_DIM), 1.0, 6.0, ((0, 32),))
    saved_output = gaussian(arg_keys[3], (TOK, KV_HEADS * GROUP * HEAD_DIM), 0.1, 0.59765625, ((0, 32),))
    output_grad = gaussian(arg_keys[4], (TOK, KV_HEADS * GROUP * HEAD_DIM), 1.0, 6.0, ((0, 32),))
    normalizer = draw_normalizer(jax.random.fold_in(arg_keys[7], 71), 0)
    doc_lengths = draw_doc_lengths(jax.random.fold_in(arg_keys[7], 71), 0)
    return {"query_states": query_states, "key_states": key_states, "value_states": value_states, "saved_output": saved_output, "output_grad": output_grad, "normalizer": normalizer, "doc_lengths": doc_lengths}


def document_ids(doc_lengths, positions):
    doc_ends = jnp.cumsum(doc_lengths)
    return jnp.sum((positions[:, None] >= doc_ends[None, :]).astype(jnp.int32), axis=1)


def reference(query_states, key_states, value_states, saved_output, output_grad, normalizer, doc_lengths):
    scaling = HEAD_DIM ** -0.5
    head_count = KV_HEADS * GROUP
    positions = jnp.arange(TOK, dtype=jnp.int32)
    documents = document_ids(doc_lengths, positions)
    row_delta = jnp.sum((output_grad.astype(jnp.float32) * saved_output.astype(jnp.float32)).reshape(TOK, head_count, HEAD_DIM), axis=2)
    block_rows = 512 if TOK % 512 == 0 else TOK
    block_count = TOK // block_rows
    window = min(block_rows + MOST, TOK)
    query_heads = query_states.astype(jnp.float32).reshape(TOK, KV_HEADS, GROUP, HEAD_DIM).transpose(1, 0, 2, 3)
    grad_heads = output_grad.astype(jnp.float32).reshape(TOK, KV_HEADS, GROUP, HEAD_DIM).transpose(1, 0, 2, 3)
    key_heads = key_states.astype(jnp.float32).reshape(TOK, KV_HEADS, HEAD_DIM).transpose(1, 0, 2)
    value_heads = value_states.astype(jnp.float32).reshape(TOK, KV_HEADS, HEAD_DIM).transpose(1, 0, 2)
    norm_heads = normalizer.reshape(TOK, KV_HEADS, GROUP).transpose(1, 0, 2)
    delta_heads = row_delta.reshape(TOK, KV_HEADS, GROUP).transpose(1, 0, 2)

    def one_head(operands):
        query_all, grad_all, key_all, value_all, norm_all, delta_all = operands

        def one_block(running, block_index):
            key_acc, value_acc = running
            start_row = block_index * block_rows
            key_start = jnp.clip(start_row - MOST, 0, TOK - window).astype(jnp.int32)
            query_rows = lax.dynamic_slice_in_dim(query_all, start_row, block_rows, 0)
            grad_rows = lax.dynamic_slice_in_dim(grad_all, start_row, block_rows, 0)
            norm_rows = lax.dynamic_slice_in_dim(norm_all, start_row, block_rows, 0)
            delta_rows = lax.dynamic_slice_in_dim(delta_all, start_row, block_rows, 0)
            key_rows = lax.dynamic_slice_in_dim(key_all, key_start, window, 0)
            value_rows = lax.dynamic_slice_in_dim(value_all, key_start, window, 0)
            key_pos = lax.dynamic_slice_in_dim(positions, key_start, window, 0)
            key_doc = lax.dynamic_slice_in_dim(documents, key_start, window, 0)
            query_pos = start_row + jnp.arange(block_rows, dtype=jnp.int32)
            query_doc = lax.dynamic_slice_in_dim(documents, start_row, block_rows, 0)
            allowed = (key_pos[None, :] <= query_pos[:, None]) & (key_doc[None, :] == query_doc[:, None])
            scores = jnp.einsum("qgd,kd->gqk", query_rows, key_rows) * scaling
            probability = jnp.where(allowed[None], jnp.exp(scores - norm_rows.T[:, :, None]), 0.0)
            prob_grad = jnp.einsum("qgd,kd->gqk", grad_rows, value_rows)
            score_grad = probability * (prob_grad - delta_rows.T[:, :, None])
            prob_half = lax.optimization_barrier(probability.astype(jnp.bfloat16)).astype(jnp.float32)
            grad_half = lax.optimization_barrier(score_grad.astype(jnp.bfloat16)).astype(jnp.float32)
            value_add = jnp.einsum("gqk,qgd->kd", prob_half, grad_rows)
            key_add = jnp.einsum("gqk,qgd->kd", grad_half, query_rows)
            value_acc = lax.dynamic_update_slice_in_dim(value_acc, lax.dynamic_slice_in_dim(value_acc, key_start, window, 0) + value_add, key_start, 0)
            key_acc = lax.dynamic_update_slice_in_dim(key_acc, lax.dynamic_slice_in_dim(key_acc, key_start, window, 0) + key_add, key_start, 0)
            query_part = jnp.einsum("gqk,kd->qgd", grad_half, key_rows) * scaling
            return (key_acc, value_acc), query_part

        empty_rows = jnp.zeros((TOK, HEAD_DIM), jnp.float32)
        (key_acc, value_acc), query_parts = lax.scan(one_block, (empty_rows, empty_rows), jnp.arange(block_count, dtype=jnp.int32))
        return query_parts.reshape(TOK, GROUP, HEAD_DIM), key_acc * scaling, value_acc

    query_all_grad, key_all_grad, value_all_grad = lax.map(one_head, (query_heads, grad_heads, key_heads, value_heads, norm_heads, delta_heads))
    query_grad = query_all_grad.transpose(1, 0, 2, 3).reshape(TOK, head_count * HEAD_DIM).astype(jnp.bfloat16)
    key_grad = key_all_grad.transpose(1, 0, 2).reshape(TOK, KV_HEADS * HEAD_DIM).astype(jnp.bfloat16)
    value_grad = value_all_grad.transpose(1, 0, 2).reshape(TOK, KV_HEADS * HEAD_DIM).astype(jnp.bfloat16)
    return (query_grad, key_grad, value_grad)
```

```python
import functools
import math

import jax
import jax.numpy as jnp
from jax import lax
from jax.experimental import pallas as pl
from jax.experimental.pallas import tpu as pltpu
from jax.sharding import Mesh, PartitionSpec as P

HEAD_DIM = 128
KV_HEADS = 4
MOST = 8192
SCALING = HEAD_DIM ** (-0.5)
LOG2E = math.log2(math.e)
MESH = pl.DeviceIdType.MESH
TILE_K = 512


def dot(a, b, dims):
    return lax.dot_general(a, b, (dims, ((), ())), preferred_element_type=jnp.float32)


def spread_kernel(
    planes, q_ref, g_ref, nd_ref, k_ref, v_ref, qo, go, ndo, ko, vo,
    send, recv, relay, kv_send, kv_recv, fwd_send, fwd_recv,
):
    row = lax.axis_index("qrow")
    z = lax.axis_index("kcol")
    s = row // 2
    core = row % 2
    tile = q_ref.shape[0] // 2
    heads = KV_HEADS
    partner = s * 2 + 1 - core
    below = jnp.minimum(jnp.maximum(s - z, 0), 1)
    plane = s - below
    slot = core * planes + z

    def query_parts(h, half):
        rows = pl.ds(half * tile, tile)
        cols = pl.ds(pl.multiple_of(h * HEAD_DIM, HEAD_DIM), HEAD_DIM)
        return q_ref.at[rows, cols], g_ref.at[rows, cols], nd_ref.at[h, half]

    def query_dst(which, j):
        return qo.at[which, j], go.at[which, j], ndo.at[which, j]

    def query_send(i, half, act):
        h = (s + i) % heads
        to = h * 2 + (z + half) % 2
        home = (to == row) & (plane == z)
        for t, (a, b) in enumerate(zip(query_parts(h, half), query_dst(below, slot))):
            there = pltpu.make_async_remote_copy(
                a, b, send.at[t, i, half], recv.at[t, below, slot],
                device_id=(to, plane), device_id_type=MESH)
            if act == "start":
                pl.when(home)(pltpu.make_async_copy(a, b, recv.at[t, below, slot]).start)
                pl.when(jnp.logical_not(home))(there.start)
            else:
                pl.when(jnp.logical_not(home))(there.wait_send)

    def key_send(i, act):
        h = (s + i) % heads
        cols = pl.ds(pl.multiple_of(h * HEAD_DIM, HEAD_DIM), HEAD_DIM)
        for t, (a, b) in enumerate(((k_ref, ko), (v_ref, vo))):
            if i == 0:
                if act == "start":
                    pltpu.make_async_copy(a.at[:, cols], b.at[row], kv_recv.at[t, s]).start()
            else:
                there = pltpu.make_async_remote_copy(
                    a.at[:, cols], b.at[row], kv_send.at[t, i], kv_recv.at[t, s],
                    device_id=(h * 2 + core, z), device_id_type=MESH)
                there.start() if act == "start" else there.wait_send()

    def arrived(which, j):
        for t, b in enumerate(query_dst(which, j)):
            pltpu.make_async_copy(b, b, recv.at[t, which, j]).wait()

    def pass_on(which, j, act):
        to = z - 1 + 2 * which
        for t, (a, b) in enumerate(zip(query_dst(which, j), query_dst(1 - which, j))):
            copy = pltpu.make_async_remote_copy(
                a, b, relay.at[t, which, j], recv.at[t, 1 - which, j],
                device_id=(row, to), device_id_type=MESH)
            copy.start() if act == "start" else copy.wait_send()

    def key_forward(i, act):
        src = (s + i) % heads
        for t, b in enumerate((ko, vo)):
            at = b.at[src * 2 + core]
            copy = pltpu.make_async_remote_copy(
                at, at, fwd_send.at[t, i], fwd_recv.at[t, src],
                device_id=(partner, z), device_id_type=MESH)
            if act == "start":
                pltpu.make_async_copy(at, at, kv_recv.at[t, src]).wait()
                copy.start()
            else:
                copy.wait_send()
                got = b.at[src * 2 + 1 - core]
                pltpu.make_async_copy(got, got, fwd_recv.at[t, src]).wait()

    for i in range(heads):
        for half in range(2):
            query_send(i, half, "start")
        key_send(i, "start")

    def direct(j, z0, act):
        @pl.when((z0 >= z))
        def _():
            if act == "start":
                arrived(0, j)

            @pl.when(z >= 1)
            def _():
                pass_on(0, j, act)

        @pl.when((z0 <= z) & (z + 1 < planes))
        def _():
            if act == "start":
                arrived(1, j)
            pass_on(1, j, act)

    for z0 in range(planes):
        for c0 in range(2):
            direct(c0 * planes + z0, z0, "start")
    for i in range(heads):
        key_forward(i, "start")
    for z0 in range(planes):
        for c0 in range(2):
            j = c0 * planes + z0
            pl.when(z0 < z)(functools.partial(arrived, 0, j))
            pl.when((z0 > z) & (z + 1 < planes))(functools.partial(arrived, 1, j))
    for i in range(heads):
        for half in range(2):
            query_send(i, half, "wait")
        key_send(i, "wait")
        key_forward(i, "wait")
    for z0 in range(planes):
        for c0 in range(2):
            direct(c0 * planes + z0, z0, "wait")


def spread(planes, q, g, nd, k, v):
    n = q.shape[0]
    slots = 2 * planes
    anywhere = pl.BlockSpec(memory_space=pl.ANY)
    whole = pl.BlockSpec(memory_space=pltpu.VMEM)
    dma = pltpu.SemaphoreType.DMA
    tiles = jax.ShapeDtypeStruct((2, slots, n // 2, HEAD_DIM), jnp.bfloat16)
    keys = jax.ShapeDtypeStruct((2 * KV_HEADS, n, HEAD_DIM), jnp.bfloat16)
    return pl.pallas_call(
        functools.partial(spread_kernel, planes),
        out_shape=(tiles, tiles, jax.ShapeDtypeStruct((2, slots, 2, n // 2), jnp.float32), keys, keys),
        in_specs=[anywhere] * 5,
        out_specs=(whole,) * 5,
        scratch_shapes=[
            dma((3, KV_HEADS, 2)), dma((3, 2, slots)), dma((3, 2, slots)),
            dma((2, KV_HEADS)), dma((2, KV_HEADS)), dma((2, KV_HEADS)), dma((2, KV_HEADS)),
        ],
        compiler_params=pltpu.CompilerParams(
            has_side_effects=True, vmem_limit_bytes=40 * 1024 * 1024),
        name="spread",
    )(q, g, nd, k, v)


def attention_kernel(
    docs, ends_ref, q_ref, g_ref, nd_ref, k_ref, v_ref, dq_ref, dk_ref, dv_ref,
    dq_acc, dk_acc, dv_acc,
):
    slots, tile_q = q_ref.shape[1], q_ref.shape[2]
    segment = dk_acc.shape[0]
    tile_k = dk_tile = min(TILE_K, segment)
    core = lax.axis_index("qrow") % 2
    base = lax.axis_index("kcol") * segment

    def doc_start(position):
        start = jnp.zeros_like(position)
        for d in range(docs):
            start = jnp.where(position >= ends_ref[d], ends_ref[d], start)
        return start

    dk_acc[...] = jnp.zeros_like(dk_acc)
    dv_acc[...] = jnp.zeros_like(dv_acc)

    def query_step(i, carry):
        which = i // slots
        j = i % slots
        q_lo = which * segment + (2 * j + (core + j) % 2) * tile_q
        q_pos = q_lo + lax.broadcasted_iota(jnp.int32, (1, tile_q), 1)
        q_start = doc_start(q_pos + base) - base
        lo = jnp.maximum(doc_start(q_lo + base) - base, 0)
        hi = jnp.minimum(q_lo + tile_q, segment)
        last_start = jnp.maximum(doc_start(q_lo + base + tile_q - 1) - base, 0)
        first = lo // tile_k
        last = (hi + tile_k - 1) // tile_k
        full_lo = jnp.minimum((last_start + tile_k - 1) // tile_k, last)
        full_hi = jnp.maximum(jnp.minimum((q_lo + 1) // tile_k, last), full_lo)
        q = q_ref[which, j]
        g = g_ref[which, j]
        nd = nd_ref[which, j]
        norm = nd[0:1, :]
        delta = nd[1:2, :]
        dq_acc[...] = jnp.zeros_like(dq_acc)

        def key_step(masked, kt, carry):
            rows = pl.ds(pl.multiple_of(kt * tile_k, tile_k), tile_k)
            k = k_ref[rows, :]
            v = v_ref[rows, :]
            s = dot(k, q, ((1,), (1,)))
            dp = dot(v, g, ((1,), (1,)))
            p = jnp.exp2(s * (SCALING * LOG2E) - norm)
            if masked:
                k_pos = kt * tile_k + lax.broadcasted_iota(jnp.int32, (tile_k, 1), 0)
                p = jnp.where((k_pos <= q_pos) & (k_pos >= q_start), p, 0.0)
            ds = (p * (dp - delta)).astype(jnp.bfloat16)
            dv_acc[rows, :] += dot(p.astype(jnp.bfloat16), g, ((1,), (0,)))
            dk_acc[rows, :] += dot(ds, q, ((1,), (0,)))
            dq_acc[...] += dot(k, ds, ((0,), (0,)))
            return carry

        @pl.when(lo < hi)
        def _():
            lax.fori_loop(first, full_lo, functools.partial(key_step, True), 0)
            lax.fori_loop(full_lo, full_hi, functools.partial(key_step, False), 0)
            lax.fori_loop(full_hi, last, functools.partial(key_step, True), 0)

        dq_ref[which, j] = (dq_acc[...] * SCALING).T.astype(jnp.bfloat16)
        return carry

    lax.fori_loop(0, 2 * slots, query_step, 0)

    def finish(kt, carry):
        rows = pl.ds(pl.multiple_of(kt * tile_k, tile_k), tile_k)
        dk_ref[rows, :] = (dk_acc[rows, :] * SCALING).astype(jnp.bfloat16)
        dv_ref[rows, :] = dv_acc[rows, :].astype(jnp.bfloat16)
        return carry

    lax.fori_loop(0, segment // tile_k, finish, 0)


def attention(ends, q, g, nd, k, v):
    tile_q = q.shape[2]
    segment = k.shape[0]
    whole = pl.BlockSpec(memory_space=pltpu.VMEM)
    scalars = pl.BlockSpec(memory_space=pltpu.SMEM)
    return pl.pallas_call(
        functools.partial(attention_kernel, ends.shape[0]),
        out_shape=(
            jax.ShapeDtypeStruct(q.shape, jnp.bfloat16),
            jax.ShapeDtypeStruct(k.shape, jnp.bfloat16),
            jax.ShapeDtypeStruct(v.shape, jnp.bfloat16),
        ),
        in_specs=[scalars] + [whole] * 5,
        out_specs=(whole,) * 3,
        scratch_shapes=[
            pltpu.VMEM((HEAD_DIM, tile_q), jnp.float32),
            pltpu.VMEM((segment, HEAD_DIM), jnp.float32),
            pltpu.VMEM((segment, HEAD_DIM), jnp.float32),
        ],
        compiler_params=pltpu.CompilerParams(vmem_limit_bytes=58 * 1024 * 1024),
        name="attention",
    )(ends, q, g, nd, k, v)


def collect_kernel(
    planes, dq_ref, dk_ref, dv_ref, dqo, dko, dvo, parts, pair, summed,
    send, recv, pair_send, pair_recv, kv_send, kv_recv,
):
    row = lax.axis_index("qrow")
    z = lax.axis_index("kcol")
    s = row // 2
    core = row % 2
    heads = KV_HEADS
    tile = dq_ref.shape[2]
    n = dko.shape[0]
    partner = s * 2 + 1 - core
    mine = pl.ds(pl.multiple_of(s * HEAD_DIM, HEAD_DIM), HEAD_DIM)
    kv = ((dk_ref, dko), (dv_ref, dvo))

    def trade(i, act):
        to = (s + 1 + i) % heads
        for t, (a, _) in enumerate(kv):
            copy = pltpu.make_async_remote_copy(
                a.at[to * 2 + 1 - core], pair.at[t, to], pair_send.at[t, to], pair_recv.at[t, to],
                device_id=(partner, z), device_id_type=MESH)
            copy.start() if act == "start" else copy.wait_send()

    def query_return(which, c0, z0, act):
        j = c0 * planes + z0
        half = (core + z0) % 2
        to = (z + which) * 2 + c0
        home = (to == row) & (z0 == z)
        copy = pltpu.make_async_remote_copy(
            dq_ref.at[which, j], parts.at[which, s, half],
            send.at[which, j], recv.at[which, s, half],
            device_id=(to, z0), device_id_type=MESH)

        def move():
            if act == "start":
                @pl.when(home)
                def _():
                    parts[which, s, half] = dq_ref[which, j]
                pl.when(jnp.logical_not(home))(copy.start)
            else:
                pl.when(jnp.logical_not(home))(copy.wait_send)
        if which == 0:
            move()
        else:
            pl.when(z + 1 < planes)(move)

    def every_query(act):
        for dz in range(planes):
            for c0 in range(2):
                for which in range(2):
                    query_return(which, c0, dz, act)

    for i in range(heads):
        trade(i, "start")
    every_query("start")

    def key_return(i, act):
        to = (s + 1 + i) % heads
        if i == heads - 1 and act != "sum":
            return
        for t, (a, out) in enumerate(kv):
            if act == "sum":
                got = pair.at[t, to]
                pltpu.make_async_copy(got, got, pair_recv.at[t, to]).wait()
                total = (a[to * 2 + core].astype(jnp.float32)
                         + pair[t, to].astype(jnp.float32)).astype(jnp.bfloat16)
                if i == heads - 1:
                    out[:, mine] = total
                else:
                    summed[t, to] = total
            else:
                copy = pltpu.make_async_remote_copy(
                    summed.at[t, to], out.at[:, mine], kv_send.at[t, to], kv_recv.at[t, s],
                    device_id=(to * 2 + core, z), device_id_type=MESH)
                copy.start() if act == "start" else copy.wait_send()

    for i in range(heads):
        key_return(i, "sum")
        if i:
            key_return(i - 1, "start")

    def add_up(h, half):
        home = (h == s) & (z == s) & (half == (core + z) % 2)
        home_next = (h == s) & (s == z + 1) & (half == (core + z) % 2)
        got = parts.at[0, h, half]
        pl.when(jnp.logical_not(home))(pltpu.make_async_copy(got, got, recv.at[0, h, half]).wait)
        rows = pl.ds(half * tile, tile)
        cols = pl.ds(h * HEAD_DIM, HEAD_DIM)

        @pl.when(s == 0)
        def _():
            dqo[rows, cols] = parts[0, h, half]

        @pl.when(s > 0)
        def _():
            more = parts.at[1, h, half]
            pl.when(jnp.logical_not(home_next))(
                pltpu.make_async_copy(more, more, recv.at[1, h, half]).wait)
            dqo[rows, cols] = (parts[0, h, half].astype(jnp.float32)
                               + parts[1, h, half].astype(jnp.float32)).astype(jnp.bfloat16)

    for h in range(heads):
        for half in range(2):
            add_up(h, half)
    for i in range(heads):
        trade(i, "wait")
        key_return(i, "wait")
    every_query("wait")
    for i in range(heads - 1):
        src = (s + 1 + i) % heads
        cols = pl.ds(pl.multiple_of(src * HEAD_DIM, HEAD_DIM), HEAD_DIM)
        for t, (_, out) in enumerate(kv):
            got = out.at[:, cols]
            pltpu.make_async_copy(got, got, kv_recv.at[t, src]).wait()


def collect(planes, dq, dk, dv):
    tile = dq.shape[2]
    n = dk.shape[1]
    whole = pl.BlockSpec(memory_space=pltpu.VMEM)
    dma = pltpu.SemaphoreType.DMA
    out = jax.ShapeDtypeStruct((n, KV_HEADS * HEAD_DIM), jnp.bfloat16)
    return pl.pallas_call(
        functools.partial(collect_kernel, planes),
        out_shape=(out,) * 3,
        in_specs=[whole] * 3,
        out_specs=(whole,) * 3,
        scratch_shapes=[
            pltpu.VMEM((2, KV_HEADS, 2, tile, HEAD_DIM), jnp.bfloat16),
            pltpu.VMEM((2, KV_HEADS, n, HEAD_DIM), jnp.bfloat16),
            pltpu.VMEM((2, KV_HEADS, n, HEAD_DIM), jnp.bfloat16),
            dma((2, 2 * planes)), dma((2, KV_HEADS, 2)),
            dma((2, KV_HEADS)), dma((2, KV_HEADS)), dma((2, KV_HEADS)), dma((2, KV_HEADS)),
        ],
        compiler_params=pltpu.CompilerParams(
            has_side_effects=True, vmem_limit_bytes=40 * 1024 * 1024),
        name="collect",
    )(dq, dk, dv)


def by_segment(planes, query_states, key_states, value_states, saved_output, output_grad,
               normalizer, doc_lengths):
    n = query_states.shape[0]
    row_delta = jnp.sum(
        (output_grad.astype(jnp.float32) * saved_output.astype(jnp.float32)).reshape(
            n, KV_HEADS, HEAD_DIM
        ),
        axis=2,
    )
    nd = jnp.stack([normalizer * LOG2E, row_delta], axis=0)
    nd = nd.reshape(2, 2, n // 2, KV_HEADS).transpose(3, 1, 0, 2)
    q, g, nd, k, v = spread(planes, query_states, output_grad, nd, key_states, value_states)
    ends = jnp.cumsum(doc_lengths)
    dq, dk, dv = attention(ends, q, g, nd, k.reshape(-1, HEAD_DIM), v.reshape(-1, HEAD_DIM))
    return collect(planes, dq, dk.reshape(-1, n, HEAD_DIM), dv.reshape(-1, n, HEAD_DIM))


DEAL_Q = 512
DEAL_K = 256
Q_AXES = ("yx", "core", "ko", "head")
K_AXES = ("ko", "head", "yx", "core")


def dealt_kernel(
    piece, groups, docs, ends_ref, where_ref, q_ref, g_ref, nd_ref, k_ref, v_ref,
    dq_ref, dk_ref, dv_ref, dq_acc, dk_acc, dv_acc,
):
    tile_q = nd_ref.shape[2]
    tile_k = dk_acc.shape[0]
    q_tiles = q_ref.shape[0] // tile_q
    k_tiles = k_ref.shape[0] // tile_k
    core = where_ref[0]
    group = where_ref[1]
    run = 2 * piece

    def key_token(i):
        return (i // run) * (groups * run) + group * run + i % run

    def doc_end(position):
        end = jnp.zeros_like(position)
        for d in range(docs - 1, -1, -1):
            end = jnp.where(position < ends_ref[d], ends_ref[d], end)
        return end

    dq_acc[...] = jnp.zeros_like(dq_acc)
    q_local = lax.broadcasted_iota(jnp.int32, (1, tile_q), 1)
    q_base = (q_local // piece) * run + core * piece + q_local % piece

    def key_step(kt, carry):
        k_lo = kt * tile_k
        rows = pl.ds(pl.multiple_of(k_lo, tile_k), tile_k)
        k = k_ref[rows, :]
        v = v_ref[rows, :]
        k_t = k.T
        k_pos = key_token(k_lo + lax.broadcasted_iota(jnp.int32, (tile_k, 1), 0))
        k_end = doc_end(k_pos)
        first = key_token(k_lo) // (2 * tile_q)
        last = (doc_end(key_token(k_lo + tile_k - 1)) - 1) // (2 * tile_q)
        dk_acc[...] = jnp.zeros_like(dk_acc)
        dv_acc[...] = jnp.zeros_like(dv_acc)

        def query_step(qt, carry):
            q_rows = pl.ds(pl.multiple_of(qt * tile_q, tile_q), tile_q)
            q = q_ref[q_rows, :]
            g = g_ref[q_rows, :]
            nd = nd_ref[qt]
            norm = nd[0:1, :]
            delta = nd[1:2, :]
            q_pos = q_base + qt * (2 * tile_q)
            s = dot(k, q, ((1,), (1,)))
            dp = dot(v, g, ((1,), (1,)))
            allowed = (k_pos <= q_pos) & (q_pos < k_end)
            p = jnp.where(allowed, jnp.exp2(s * (SCALING * LOG2E) - norm), 0.0)
            ds = (p * (dp - delta)).astype(jnp.bfloat16)
            dv_acc[...] += dot(p.astype(jnp.bfloat16), g, ((1,), (0,)))
            dk_acc[...] += dot(ds, q, ((1,), (0,)))
            dq_acc[qt] += dot(k_t, ds, ((1,), (0,)))
            return carry

        lax.fori_loop(first, last + 1, query_step, 0)
        dk_ref[rows, :] = (dk_acc[...] * SCALING).astype(jnp.bfloat16)
        dv_ref[rows, :] = dv_acc[...].astype(jnp.bfloat16)
        return carry

    lax.fori_loop(0, k_tiles, key_step, 0)

    def finish(qt, carry):
        q_rows = pl.ds(pl.multiple_of(qt * tile_q, tile_q), tile_q)
        dq_ref[q_rows, :] = (dq_acc[qt] * SCALING).T.astype(jnp.bfloat16)
        return carry

    lax.fori_loop(0, q_tiles, finish, 0)


def dealt_attention(piece, groups, ends, place, q, g, nd, k, v):
    tile_q = nd.shape[2]
    tile_k = min(DEAL_K, k.shape[0])
    whole = pl.BlockSpec(memory_space=pltpu.VMEM)
    scalars = pl.BlockSpec(memory_space=pltpu.SMEM)
    return pl.pallas_call(
        functools.partial(dealt_kernel, piece, groups, ends.shape[0]),
        out_shape=(
            jax.ShapeDtypeStruct(q.shape, jnp.bfloat16),
            jax.ShapeDtypeStruct(k.shape, jnp.bfloat16),
            jax.ShapeDtypeStruct(v.shape, jnp.bfloat16),
        ),
        in_specs=[scalars, scalars, whole, whole, whole, whole, whole],
        out_specs=(whole, whole, whole),
        scratch_shapes=[
            pltpu.VMEM((q.shape[0] // tile_q, HEAD_DIM, tile_q), jnp.float32),
            pltpu.VMEM((tile_k, HEAD_DIM), jnp.float32),
            pltpu.VMEM((tile_k, HEAD_DIM), jnp.float32),
        ],
        compiler_params=pltpu.CompilerParams(vmem_limit_bytes=58 * 1024 * 1024),
    )(ends, place, q, g, nd, k, v)


def per_device(sizes, query_states, key_states, value_states, saved_output, output_grad,
               normalizer, doc_lengths):
    yx, core, ko, head = (sizes[a] for a in Q_AXES)
    devices = yx * core * ko * head
    rows = query_states.shape[0]
    piece = rows // (yx * ko * core)
    groups = yx * ko
    row_delta = jnp.sum(
        (output_grad.astype(jnp.float32) * saved_output.astype(jnp.float32)).reshape(
            rows, KV_HEADS, HEAD_DIM
        ),
        axis=2,
    )

    def deal(x, key_side):
        x = x.reshape(yx, ko, core, piece, KV_HEADS, -1)
        order = (1, 4, 0, 2, 3, 5) if key_side else (0, 2, 1, 4, 3, 5)
        x = x.transpose(order).reshape(devices, piece, x.shape[-1])
        return lax.all_to_all(x, K_AXES if key_side else Q_AXES, 0, 0, tiled=True)

    def undeal(x, key_side):
        x = lax.all_to_all(x, K_AXES if key_side else Q_AXES, 0, 0, tiled=True)
        if key_side:
            x = x.reshape(ko, head, yx, core, piece, HEAD_DIM).transpose(2, 0, 3, 4, 1, 5)
        else:
            x = x.reshape(yx, core, ko, head, piece, HEAD_DIM).transpose(0, 2, 1, 4, 3, 5)
        return x.reshape(rows, KV_HEADS * HEAD_DIM)

    nd = jnp.stack([normalizer * LOG2E, row_delta], axis=-1)
    nd = deal(nd, False)
    q = deal(query_states, False)
    g = deal(output_grad, False)
    k = deal(key_states, True)
    v = deal(value_states, True)

    def gather(x, axes):
        x = lax.all_gather(x, axes, axis=0, tiled=False)
        return x.transpose(1, 0, 2, 3).reshape(-1, x.shape[-1])

    nd = gather(nd, ("yx", "ko"))
    q = gather(q, ("yx", "ko"))
    g = gather(g, ("yx", "ko"))
    k = gather(k, ("core",))
    v = gather(v, ("core",))
    tile_q = min(DEAL_Q, q.shape[0])
    nd = nd.reshape(-1, tile_q, 2).transpose(0, 2, 1)
    place = jnp.stack(
        [lax.axis_index("core"), lax.axis_index("yx") * ko + lax.axis_index("ko")]
    ).astype(jnp.int32)
    ends = jnp.cumsum(doc_lengths)
    dq, dk, dv = dealt_attention(piece, groups, ends, place, q, g, nd, k, v)

    def total(x, parts, axes):
        x = x.reshape(devices, parts, piece, HEAD_DIM).transpose(1, 0, 2, 3)
        x = lax.all_to_all(x, axes, 0, 0, tiled=True)
        return jnp.sum(x.astype(jnp.float32), axis=0).astype(jnp.bfloat16)

    dq = undeal(total(dq, groups, ("yx", "ko")), False)
    dk = undeal(total(dk, core, ("core",)), True)
    dv = undeal(total(dv, core, ("core",)), True)
    return dq, dk, dv


def solution(mesh):
    qrow = mesh.shape["qrow"]
    kcol = mesh.shape["kcol"]

    def whole(*args):
        tokens = args[0].shape[0]
        if qrow == 2 * KV_HEADS and kcol == KV_HEADS and tokens // kcol >= MOST:
            by_query, by_key = P(("qrow", "kcol"), None), P(("kcol", "qrow"), None)
            place, body = mesh, functools.partial(by_segment, kcol)
        else:
            sizes = {"yx": qrow // 2, "core": 2, "ko": kcol // KV_HEADS, "head": KV_HEADS}
            place = Mesh(mesh.devices.reshape([sizes[a] for a in Q_AXES]), Q_AXES)
            by_query, by_key = P(Q_AXES, None), P(K_AXES, None)
            body = functools.partial(per_device, sizes)
        return jax.shard_map(
            body,
            mesh=place,
            in_specs=(by_query, by_key, by_key, by_query, by_query, by_query, P()),
            out_specs=(by_query, by_key, by_key),
            check_vma=False,
        )(*args)

    return whole
```

```python
import functools
import math

import jax
import jax.numpy as jnp
from jax import lax
from jax.experimental import pallas as pl
from jax.experimental.pallas import tpu as pltpu
from jax.sharding import Mesh, PartitionSpec as P

HEAD_DIM = 128
KV_HEADS = 4
MOST = 8192
SCALING = HEAD_DIM ** (-0.5)
LOG2E = math.log2(math.e)
MESH = pl.DeviceIdType.MESH
TILE_K = 1024


def dot(a, b, dims):
    return lax.dot_general(a, b, (dims, ((), ())), preferred_element_type=jnp.float32)


def spread_kernel(
    planes, q_ref, g_ref, nd_ref, k_ref, v_ref, qo, go, ndo, ko, vo, qs, gs, nds,
    send, recv, stage_recv, stage_send, kv_send, kv_recv, fwd_send, fwd_recv,
):
    row = lax.axis_index("qrow")
    z = lax.axis_index("kcol")
    s = row // 2
    core = row % 2
    tile = q_ref.shape[0] // 2
    heads = KV_HEADS
    partner = s * 2 + 1 - core

    def query_parts(h, half):
        rows = pl.ds(half * tile, tile)
        cols = pl.ds(pl.multiple_of(h * HEAD_DIM, HEAD_DIM), HEAD_DIM)
        return q_ref.at[rows, cols], g_ref.at[rows, cols], nd_ref.at[h, half]

    def query_dst(j):
        return qo.at[j], go.at[j], ndo.at[j]

    def staged(src, c0):
        return qs.at[src, c0], gs.at[src, c0], nds.at[src, c0]

    def query_send(i, half, act):
        h = (s + i) % heads
        to = h * 2 + (z + half) % 2
        home = to == row
        here = s == z

        def move(dst, sem):
            for t, (a, b) in enumerate(zip(query_parts(h, half), dst)):
                def remote():
                    return pltpu.make_async_remote_copy(
                        a, b, send.at[t, i, half], sem(t),
                        device_id=(to, z), device_id_type=MESH)
                if act == "start":
                    @pl.when(home)
                    def _():
                        pltpu.make_async_copy(a, b, sem(t)).start()

                    @pl.when(jnp.logical_not(home))
                    def _():
                        remote().start()
                else:
                    @pl.when(jnp.logical_not(home))
                    def _():
                        remote().wait_send()

        slot = core * planes + z

        @pl.when(here)
        def _():
            move(query_dst(slot), lambda t: recv.at[t, slot])

        @pl.when(jnp.logical_not(here))
        def _():
            move(staged(s, core), lambda t: stage_recv.at[t, s, core])

    def stage_forward(i, c0, act):
        src = (s + heads - i) % heads
        slot = c0 * planes + z

        @pl.when(src != z)
        def _():
            for t, (a, b) in enumerate(zip(staged(src, c0), query_dst(slot))):
                copy = pltpu.make_async_remote_copy(
                    a, b, stage_send.at[t, src, c0], recv.at[t, slot],
                    device_id=(row, src), device_id_type=MESH)
                if act == "start":
                    pltpu.make_async_copy(a, a, stage_recv.at[t, src, c0]).wait()
                    copy.start()
                else:
                    copy.wait_send()

    def key_send(i, act):
        h = (s + i) % heads
        cols = pl.ds(pl.multiple_of(h * HEAD_DIM, HEAD_DIM), HEAD_DIM)
        for t, (a, b) in enumerate(((k_ref, ko), (v_ref, vo))):
            if i == 0:
                if act == "start":
                    pltpu.make_async_copy(a.at[:, cols], b.at[row], kv_recv.at[t, s]).start()
            else:
                there = pltpu.make_async_remote_copy(
                    a.at[:, cols], b.at[row], kv_send.at[t, i], kv_recv.at[t, s],
                    device_id=(h * 2 + core, z), device_id_type=MESH)
                there.start() if act == "start" else there.wait_send()

    def arrived(j):
        for t, b in enumerate(query_dst(j)):
            pltpu.make_async_copy(b, b, recv.at[t, j]).wait()

    def key_forward(i, act):
        src = (s + heads - i) % heads
        for t, b in enumerate((ko, vo)):
            at = b.at[src * 2 + core]
            copy = pltpu.make_async_remote_copy(
                at, at, fwd_send.at[t, src], fwd_recv.at[t, src],
                device_id=(partner, z), device_id_type=MESH)
            if act == "start":
                pltpu.make_async_copy(at, at, kv_recv.at[t, src]).wait()
                copy.start()
            else:
                copy.wait_send()
                got = b.at[src * 2 + 1 - core]
                pltpu.make_async_copy(got, got, fwd_recv.at[t, src]).wait()

    for i in range(heads):
        for half in range(2):
            query_send(i, half, "start")
    for i in range(heads):
        key_send(i, "start")
    for i in range(heads):
        for c0 in range(2):
            stage_forward(i, c0, "start")
    for i in range(heads):
        key_forward(i, "start")
    for j in range(2 * planes):
        arrived(j)
    for i in range(heads):
        for half in range(2):
            query_send(i, half, "wait")
        key_send(i, "wait")
        key_forward(i, "wait")
        for c0 in range(2):
            stage_forward(i, c0, "wait")


def spread(planes, q, g, nd, k, v):
    n = q.shape[0]
    slots = 2 * planes
    anywhere = pl.BlockSpec(memory_space=pl.ANY)
    whole = pl.BlockSpec(memory_space=pltpu.VMEM)
    dma = pltpu.SemaphoreType.DMA
    tiles = jax.ShapeDtypeStruct((slots, n // 2, HEAD_DIM), jnp.bfloat16)
    keys = jax.ShapeDtypeStruct((2 * KV_HEADS, n, HEAD_DIM), jnp.bfloat16)
    stage = pltpu.VMEM((KV_HEADS, 2, n // 2, HEAD_DIM), jnp.bfloat16)
    return pl.pallas_call(
        functools.partial(spread_kernel, planes),
        out_shape=(tiles, tiles, jax.ShapeDtypeStruct((slots, 2, n // 2), jnp.float32), keys, keys),
        in_specs=[anywhere] * 5,
        out_specs=(whole,) * 5,
        scratch_shapes=[
            stage, stage, pltpu.VMEM((KV_HEADS, 2, 2, n // 2), jnp.float32),
            dma((3, KV_HEADS, 2)), dma((3, slots)),
            dma((3, KV_HEADS, 2)), dma((3, KV_HEADS, 2)),
            dma((2, KV_HEADS)), dma((2, KV_HEADS)), dma((2, KV_HEADS)), dma((2, KV_HEADS)),
        ],
        compiler_params=pltpu.CompilerParams(
            has_side_effects=True, vmem_limit_bytes=40 * 1024 * 1024),
        name="spread",
    )(q, g, nd, k, v)


def attention_kernel(
    which, docs, ends_ref, q_ref, g_ref, nd_ref, k_ref, v_ref, *refs,
):
    before, (dq_ref, dk_ref, dv_ref, dq_acc, dk_acc, dv_acc) = refs[:-6], refs[-6:]
    slots, tile_q = q_ref.shape[0], q_ref.shape[1]
    segment = dk_acc.shape[0]
    tile_k = dk_tile = min(TILE_K, segment)
    core = lax.axis_index("qrow") % 2
    base = lax.axis_index("kcol") * segment

    def doc_start(position):
        start = jnp.zeros_like(position)
        for d in range(docs):
            start = jnp.where(position >= ends_ref[d], ends_ref[d], start)
        return start

    for i, acc in enumerate((dk_acc, dv_acc)):
        acc[...] = before[i][...].astype(jnp.float32) if before else jnp.zeros_like(acc)

    def query_step(j, carry):
        q_lo = which * segment + (2 * j + (core + j) % 2) * tile_q
        q_pos = q_lo + lax.broadcasted_iota(jnp.int32, (1, tile_q), 1)
        q_start = doc_start(q_pos + base) - base
        lo = jnp.maximum(doc_start(q_lo + base) - base, 0)
        hi = jnp.minimum(q_lo + tile_q, segment)
        last_start = jnp.maximum(doc_start(q_lo + base + tile_q - 1) - base, 0)
        first = lo // tile_k
        last = (hi + tile_k - 1) // tile_k
        full_lo = jnp.minimum((last_start + tile_k - 1) // tile_k, last)
        full_hi = jnp.maximum(jnp.minimum((q_lo + 1) // tile_k, last), full_lo)
        q = q_ref[j]
        g = g_ref[j]
        nd = nd_ref[j]
        norm = nd[0:1, :]
        delta = nd[1:2, :]
        dq_acc[...] = jnp.zeros_like(dq_acc)

        def key_step(masked, kt, carry):
            rows = pl.ds(pl.multiple_of(kt * tile_k, tile_k), tile_k)
            k = k_ref[rows, :]
            v = v_ref[rows, :]
            s = dot(k, q, ((1,), (1,)))
            dp = dot(v, g, ((1,), (1,)))
            p = jnp.exp2(s * (SCALING * LOG2E) - norm)
            if masked:
                k_pos = kt * tile_k + lax.broadcasted_iota(jnp.int32, (tile_k, 1), 0)
                p = jnp.where((k_pos <= q_pos) & (k_pos >= q_start), p, 0.0)
            ds = (p * (dp - delta)).astype(jnp.bfloat16)
            dv_acc[rows, :] += dot(p.astype(jnp.bfloat16), g, ((1,), (0,)))
            dk_acc[rows, :] += dot(ds, q, ((1,), (0,)))
            dq_acc[...] += dot(k, ds, ((0,), (0,)))
            return carry

        @pl.when(lo < hi)
        def _():
            lax.fori_loop(first, full_lo, functools.partial(key_step, True), 0)
            lax.fori_loop(full_lo, full_hi, functools.partial(key_step, False), 0)
            lax.fori_loop(full_hi, last, functools.partial(key_step, True), 0)

        dq_ref[j] = (dq_acc[...] * SCALING).T.astype(jnp.bfloat16)
        return carry

    lax.fori_loop(0, slots, query_step, 0)

    def finish(kt, carry):
        rows = pl.ds(pl.multiple_of(kt * tile_k, tile_k), tile_k)
        dk_ref[rows, :] = (dk_acc[rows, :] * (SCALING if before else 1.0)).astype(jnp.bfloat16)
        dv_ref[rows, :] = dv_acc[rows, :].astype(jnp.bfloat16)
        return carry

    lax.fori_loop(0, segment // tile_k, finish, 0)


def attention(which, ends, q, g, nd, k, v, *before):
    slots, tile_q = q.shape[:2]
    segment = k.shape[0]
    whole = pl.BlockSpec(memory_space=pltpu.VMEM)
    scalars = pl.BlockSpec(memory_space=pltpu.SMEM)
    return pl.pallas_call(
        functools.partial(attention_kernel, which, ends.shape[0]),
        out_shape=(
            jax.ShapeDtypeStruct(q.shape, jnp.bfloat16),
            jax.ShapeDtypeStruct(k.shape, jnp.bfloat16),
            jax.ShapeDtypeStruct(v.shape, jnp.bfloat16),
        ),
        in_specs=[scalars] + [whole] * (5 + len(before)),
        out_specs=(whole,) * 3,
        scratch_shapes=[
            pltpu.VMEM((HEAD_DIM, tile_q), jnp.float32),
            pltpu.VMEM((segment, HEAD_DIM), jnp.float32),
            pltpu.VMEM((segment, HEAD_DIM), jnp.float32),
        ],
        compiler_params=pltpu.CompilerParams(vmem_limit_bytes=58 * 1024 * 1024),
        cost_estimate=pl.CostEstimate(
            flops=5 * slots * tile_q * segment * HEAD_DIM, bytes_accessed=0, transcendentals=0),
        name=("attention_own", "attention_next")[which],
    )(ends, q, g, nd, k, v, *before)


def collect_kernel(
    planes, dq_own, dq_next, dk_ref, dv_ref, dqo, dko, dvo, parts, pair, summed,
    send, recv, pair_send, pair_recv, kv_send, kv_recv,
):
    row = lax.axis_index("qrow")
    z = lax.axis_index("kcol")
    s = row // 2
    core = row % 2
    heads = KV_HEADS
    tile = dq_own.shape[1]
    n = dko.shape[0]
    partner = s * 2 + 1 - core
    mine = pl.ds(pl.multiple_of(s * HEAD_DIM, HEAD_DIM), HEAD_DIM)
    kv = ((dk_ref, dko), (dv_ref, dvo))

    def trade(i, act):
        to = (s + 1 + i) % heads
        for t, (a, _) in enumerate(kv):
            copy = pltpu.make_async_remote_copy(
                a.at[to * 2 + 1 - core], pair.at[t, to], pair_send.at[t, to], pair_recv.at[t, to],
                device_id=(partner, z), device_id_type=MESH)
            copy.start() if act == "start" else copy.wait_send()

    def query_return(which, c0, z0, act):
        j = c0 * planes + z0
        half = (core + z0) % 2
        dq_ref = (dq_own, dq_next)[which]
        to = (z + which) * 2 + c0
        home = (to == row) & (z0 == z)
        copy = pltpu.make_async_remote_copy(
            dq_ref.at[j], parts.at[which, s, half],
            send.at[which, j], recv.at[which, s, half],
            device_id=(to, z0), device_id_type=MESH)

        def move():
            if act == "start":
                @pl.when(home)
                def _():
                    parts[which, s, half] = dq_ref[j]
                pl.when(jnp.logical_not(home))(copy.start)
            else:
                pl.when(jnp.logical_not(home))(copy.wait_send)
        if which == 0:
            move()
        else:
            pl.when(z + 1 < planes)(move)

    def every_query(act):
        for dz in range(planes):
            for c0 in range(2):
                for which in range(2):
                    query_return(which, c0, dz, act)

    for i in range(heads):
        trade(i, "start")
    every_query("start")

    def key_return(i, act):
        to = (s + 1 + i) % heads
        if i == heads - 1 and act != "sum":
            return
        for t, (a, out) in enumerate(kv):
            if act == "sum":
                got = pair.at[t, to]
                pltpu.make_async_copy(got, got, pair_recv.at[t, to]).wait()
                total = (a[to * 2 + core].astype(jnp.float32)
                         + pair[t, to].astype(jnp.float32)).astype(jnp.bfloat16)
                if i == heads - 1:
                    out[:, mine] = total
                else:
                    summed[t, to] = total
            else:
                copy = pltpu.make_async_remote_copy(
                    summed.at[t, to], out.at[:, mine], kv_send.at[t, to], kv_recv.at[t, s],
                    device_id=(to * 2 + core, z), device_id_type=MESH)
                copy.start() if act == "start" else copy.wait_send()

    for i in range(heads):
        key_return(i, "sum")
        if i:
            key_return(i - 1, "start")

    def add_up(h, half):
        home = (h == s) & (z == s) & (half == (core + z) % 2)
        home_next = (h == s) & (s == z + 1) & (half == (core + z) % 2)
        got = parts.at[0, h, half]
        pl.when(jnp.logical_not(home))(pltpu.make_async_copy(got, got, recv.at[0, h, half]).wait)
        rows = pl.ds(half * tile, tile)
        cols = pl.ds(h * HEAD_DIM, HEAD_DIM)

        @pl.when(s == 0)
        def _():
            dqo[rows, cols] = parts[0, h, half]

        @pl.when(s > 0)
        def _():
            more = parts.at[1, h, half]
            pl.when(jnp.logical_not(home_next))(
                pltpu.make_async_copy(more, more, recv.at[1, h, half]).wait)
            dqo[rows, cols] = (parts[0, h, half].astype(jnp.float32)
                               + parts[1, h, half].astype(jnp.float32)).astype(jnp.bfloat16)

    for h in range(heads):
        for half in range(2):
            add_up(h, half)
    for i in range(heads):
        trade(i, "wait")
        key_return(i, "wait")
    every_query("wait")
    for i in range(heads - 1):
        src = (s + 1 + i) % heads
        cols = pl.ds(pl.multiple_of(src * HEAD_DIM, HEAD_DIM), HEAD_DIM)
        for t, (_, out) in enumerate(kv):
            got = out.at[:, cols]
            pltpu.make_async_copy(got, got, kv_recv.at[t, src]).wait()


def collect(planes, dq, dq_next, dk, dv):
    tile = dq.shape[1]
    n = dk.shape[1]
    whole = pl.BlockSpec(memory_space=pltpu.VMEM)
    dma = pltpu.SemaphoreType.DMA
    out = jax.ShapeDtypeStruct((n, KV_HEADS * HEAD_DIM), jnp.bfloat16)
    return pl.pallas_call(
        functools.partial(collect_kernel, planes),
        out_shape=(out,) * 3,
        in_specs=[whole] * 4,
        out_specs=(whole,) * 3,
        scratch_shapes=[
            pltpu.VMEM((2, KV_HEADS, 2, tile, HEAD_DIM), jnp.bfloat16),
            pltpu.VMEM((2, KV_HEADS, n, HEAD_DIM), jnp.bfloat16),
            pltpu.VMEM((2, KV_HEADS, n, HEAD_DIM), jnp.bfloat16),
            dma((2, 2 * planes)), dma((2, KV_HEADS, 2)),
            dma((2, KV_HEADS)), dma((2, KV_HEADS)), dma((2, KV_HEADS)), dma((2, KV_HEADS)),
        ],
        compiler_params=pltpu.CompilerParams(
            has_side_effects=True, vmem_limit_bytes=40 * 1024 * 1024),
        name="collect",
    )(dq, dq_next, dk, dv)


def by_segment(planes, query_states, key_states, value_states, saved_output, output_grad,
               normalizer, doc_lengths):
    n = query_states.shape[0]
    row_delta = jnp.sum(
        (output_grad.astype(jnp.float32) * saved_output.astype(jnp.float32)).reshape(
            n, KV_HEADS, HEAD_DIM
        ),
        axis=2,
    )
    nd = jnp.stack([normalizer * LOG2E, row_delta], axis=0)
    nd = nd.reshape(2, 2, n // 2, KV_HEADS).transpose(3, 1, 0, 2)
    q, g, nd, k, v = spread(planes, query_states, output_grad, nd, key_states, value_states)
    ends = jnp.cumsum(doc_lengths)
    k, v = k.reshape(-1, HEAD_DIM), v.reshape(-1, HEAD_DIM)
    down = [(i + 1, i) for i in range(planes - 1)]
    shifted = [lax.ppermute(x, "kcol", down) for x in (q, g, nd)]
    dq, dk, dv = attention(0, ends, q, g, nd, k, v)
    dq_next, dk, dv = attention(1, ends, *shifted, k, v, dk, dv)
    return collect(planes, dq, dq_next, dk.reshape(-1, n, HEAD_DIM), dv.reshape(-1, n, HEAD_DIM))


DEAL_Q = 512
DEAL_K = 256
Q_AXES = ("yx", "core", "ko", "head")
K_AXES = ("ko", "head", "yx", "core")


def dealt_kernel(
    piece, groups, docs, ends_ref, where_ref, q_ref, g_ref, nd_ref, k_ref, v_ref,
    dq_ref, dk_ref, dv_ref, dq_acc, dk_acc, dv_acc,
):
    tile_q = nd_ref.shape[2]
    tile_k = dk_acc.shape[0]
    q_tiles = q_ref.shape[0] // tile_q
    k_tiles = k_ref.shape[0] // tile_k
    core = where_ref[0]
    group = where_ref[1]
    run = 2 * piece

    def key_token(i):
        return (i // run) * (groups * run) + group * run + i % run

    def doc_end(position):
        end = jnp.zeros_like(position)
        for d in range(docs - 1, -1, -1):
            end = jnp.where(position < ends_ref[d], ends_ref[d], end)
        return end

    dq_acc[...] = jnp.zeros_like(dq_acc)
    q_local = lax.broadcasted_iota(jnp.int32, (1, tile_q), 1)
    q_base = (q_local // piece) * run + core * piece + q_local % piece

    def key_step(kt, carry):
        k_lo = kt * tile_k
        rows = pl.ds(pl.multiple_of(k_lo, tile_k), tile_k)
        k = k_ref[rows, :]
        v = v_ref[rows, :]
        k_t = k.T
        k_pos = key_token(k_lo + lax.broadcasted_iota(jnp.int32, (tile_k, 1), 0))
        k_end = doc_end(k_pos)
        first = key_token(k_lo) // (2 * tile_q)
        last = (doc_end(key_token(k_lo + tile_k - 1)) - 1) // (2 * tile_q)
        dk_acc[...] = jnp.zeros_like(dk_acc)
        dv_acc[...] = jnp.zeros_like(dv_acc)

        def query_step(qt, carry):
            q_rows = pl.ds(pl.multiple_of(qt * tile_q, tile_q), tile_q)
            q = q_ref[q_rows, :]
            g = g_ref[q_rows, :]
            nd = nd_ref[qt]
            norm = nd[0:1, :]
            delta = nd[1:2, :]
            q_pos = q_base + qt * (2 * tile_q)
            s = dot(k, q, ((1,), (1,)))
            dp = dot(v, g, ((1,), (1,)))
            allowed = (k_pos <= q_pos) & (q_pos < k_end)
            p = jnp.where(allowed, jnp.exp2(s * (SCALING * LOG2E) - norm), 0.0)
            ds = (p * (dp - delta)).astype(jnp.bfloat16)
            dv_acc[...] += dot(p.astype(jnp.bfloat16), g, ((1,), (0,)))
            dk_acc[...] += dot(ds, q, ((1,), (0,)))
            dq_acc[qt] += dot(k_t, ds, ((1,), (0,)))
            return carry

        lax.fori_loop(first, last + 1, query_step, 0)
        dk_ref[rows, :] = (dk_acc[...] * SCALING).astype(jnp.bfloat16)
        dv_ref[rows, :] = dv_acc[...].astype(jnp.bfloat16)
        return carry

    lax.fori_loop(0, k_tiles, key_step, 0)

    def finish(qt, carry):
        q_rows = pl.ds(pl.multiple_of(qt * tile_q, tile_q), tile_q)
        dq_ref[q_rows, :] = (dq_acc[qt] * SCALING).T.astype(jnp.bfloat16)
        return carry

    lax.fori_loop(0, q_tiles, finish, 0)


def dealt_attention(piece, groups, ends, place, q, g, nd, k, v):
    tile_q = nd.shape[2]
    tile_k = min(DEAL_K, k.shape[0])
    whole = pl.BlockSpec(memory_space=pltpu.VMEM)
    scalars = pl.BlockSpec(memory_space=pltpu.SMEM)
    return pl.pallas_call(
        functools.partial(dealt_kernel, piece, groups, ends.shape[0]),
        out_shape=(
            jax.ShapeDtypeStruct(q.shape, jnp.bfloat16),
            jax.ShapeDtypeStruct(k.shape, jnp.bfloat16),
            jax.ShapeDtypeStruct(v.shape, jnp.bfloat16),
        ),
        in_specs=[scalars, scalars, whole, whole, whole, whole, whole],
        out_specs=(whole, whole, whole),
        scratch_shapes=[
            pltpu.VMEM((q.shape[0] // tile_q, HEAD_DIM, tile_q), jnp.float32),
            pltpu.VMEM((tile_k, HEAD_DIM), jnp.float32),
            pltpu.VMEM((tile_k, HEAD_DIM), jnp.float32),
        ],
        compiler_params=pltpu.CompilerParams(vmem_limit_bytes=58 * 1024 * 1024),
    )(ends, place, q, g, nd, k, v)


def per_device(sizes, query_states, key_states, value_states, saved_output, output_grad,
               normalizer, doc_lengths):
    yx, core, ko, head = (sizes[a] for a in Q_AXES)
    devices = yx * core * ko * head
    rows = query_states.shape[0]
    piece = rows // (yx * ko * core)
    groups = yx * ko
    row_delta = jnp.sum(
        (output_grad.astype(jnp.float32) * saved_output.astype(jnp.float32)).reshape(
            rows, KV_HEADS, HEAD_DIM
        ),
        axis=2,
    )

    def deal(x, key_side):
        x = x.reshape(yx, ko, core, piece, KV_HEADS, -1)
        order = (1, 4, 0, 2, 3, 5) if key_side else (0, 2, 1, 4, 3, 5)
        x = x.transpose(order).reshape(devices, piece, x.shape[-1])
        return lax.all_to_all(x, K_AXES if key_side else Q_AXES, 0, 0, tiled=True)

    def undeal(x, key_side):
        x = lax.all_to_all(x, K_AXES if key_side else Q_AXES, 0, 0, tiled=True)
        if key_side:
            x = x.reshape(ko, head, yx, core, piece, HEAD_DIM).transpose(2, 0, 3, 4, 1, 5)
        else:
            x = x.reshape(yx, core, ko, head, piece, HEAD_DIM).transpose(0, 2, 1, 4, 3, 5)
        return x.reshape(rows, KV_HEADS * HEAD_DIM)

    nd = jnp.stack([normalizer * LOG2E, row_delta], axis=-1)
    nd = deal(nd, False)
    q = deal(query_states, False)
    g = deal(output_grad, False)
    k = deal(key_states, True)
    v = deal(value_states, True)

    def gather(x, axes):
        x = lax.all_gather(x, axes, axis=0, tiled=False)
        return x.transpose(1, 0, 2, 3).reshape(-1, x.shape[-1])

    nd = gather(nd, ("yx", "ko"))
    q = gather(q, ("yx", "ko"))
    g = gather(g, ("yx", "ko"))
    k = gather(k, ("core",))
    v = gather(v, ("core",))
    tile_q = min(DEAL_Q, q.shape[0])
    nd = nd.reshape(-1, tile_q, 2).transpose(0, 2, 1)
    place = jnp.stack(
        [lax.axis_index("core"), lax.axis_index("yx") * ko + lax.axis_index("ko")]
    ).astype(jnp.int32)
    ends = jnp.cumsum(doc_lengths)
    dq, dk, dv = dealt_attention(piece, groups, ends, place, q, g, nd, k, v)

    def total(x, parts, axes):
        x = x.reshape(devices, parts, piece, HEAD_DIM).transpose(1, 0, 2, 3)
        x = lax.all_to_all(x, axes, 0, 0, tiled=True)
        return jnp.sum(x.astype(jnp.float32), axis=0).astype(jnp.bfloat16)

    dq = undeal(total(dq, groups, ("yx", "ko")), False)
    dk = undeal(total(dk, core, ("core",)), True)
    dv = undeal(total(dv, core, ("core",)), True)
    return dq, dk, dv


def solution(mesh):
    qrow = mesh.shape["qrow"]
    kcol = mesh.shape["kcol"]

    def whole(*args):
        tokens = args[0].shape[0]
        if qrow == 2 * KV_HEADS and kcol == KV_HEADS and tokens // kcol >= MOST:
            by_query, by_key = P(("qrow", "kcol"), None), P(("kcol", "qrow"), None)
            place, body = mesh, functools.partial(by_segment, kcol)
        else:
            sizes = {"yx": qrow // 2, "core": 2, "ko": kcol // KV_HEADS, "head": KV_HEADS}
            place = Mesh(mesh.devices.reshape([sizes[a] for a in Q_AXES]), Q_AXES)
            by_query, by_key = P(Q_AXES, None), P(K_AXES, None)
            body = functools.partial(per_device, sizes)
        return jax.shard_map(
            body,
            mesh=place,
            in_specs=(by_query, by_key, by_key, by_query, by_query, by_query, P()),
            out_specs=(by_query, by_key, by_key),
            check_vma=False,
        )(*args)

    return whole
```

```python
import functools
import math

import jax
import jax.numpy as jnp
from jax import lax
from jax.experimental import pallas as pl
from jax.experimental.pallas import tpu as pltpu
from jax.sharding import Mesh, PartitionSpec as P

HEAD_DIM = 128
KV_HEADS = 4
MOST = 8192
SCALING = HEAD_DIM ** (-0.5)
LOG2E = math.log2(math.e)
MESH = pl.DeviceIdType.MESH
TILE_K = 1024


def dot(a, b, dims):
    return lax.dot_general(a, b, (dims, ((), ())), preferred_element_type=jnp.float32)


def spread_kernel(
    planes, q_ref, g_ref, nd_ref, k_ref, v_ref, qo, go, ndo, ko, vo, qs, gs, nds,
    send, recv, stage_recv, stage_send, kv_send, kv_recv, fwd_send, fwd_recv,
):
    row = lax.axis_index("qrow")
    z = lax.axis_index("kcol")
    s = row // 2
    core = row % 2
    tile = q_ref.shape[0] // 2
    heads = KV_HEADS
    partner = s * 2 + 1 - core

    def query_parts(h, half):
        rows = pl.ds(half * tile, tile)
        cols = pl.ds(pl.multiple_of(h * HEAD_DIM, HEAD_DIM), HEAD_DIM)
        return q_ref.at[rows, cols], g_ref.at[rows, cols], nd_ref.at[h, half]

    def query_dst(j):
        return qo.at[j], go.at[j], ndo.at[j]

    def staged(src, c0):
        return qs.at[src, c0], gs.at[src, c0], nds.at[src, c0]

    def query_send(i, half, act):
        h = (s + i) % heads
        to = h * 2 + (z + half) % 2
        home = to == row
        here = s == z

        def move(dst, sem):
            for t, (a, b) in enumerate(zip(query_parts(h, half), dst)):
                def remote():
                    return pltpu.make_async_remote_copy(
                        a, b, send.at[t, i, half], sem(t),
                        device_id=(to, z), device_id_type=MESH)
                if act == "start":
                    @pl.when(home)
                    def _():
                        pltpu.make_async_copy(a, b, sem(t)).start()

                    @pl.when(jnp.logical_not(home))
                    def _():
                        remote().start()
                else:
                    @pl.when(jnp.logical_not(home))
                    def _():
                        remote().wait_send()

        slot = core * planes + z

        @pl.when(here)
        def _():
            move(query_dst(slot), lambda t: recv.at[t, slot])

        @pl.when(jnp.logical_not(here))
        def _():
            move(staged(s, core), lambda t: stage_recv.at[t, s, core])

    def stage_forward(i, c0, act):
        src = (s + heads - i) % heads
        slot = c0 * planes + z

        @pl.when(src != z)
        def _():
            for t, (a, b) in enumerate(zip(staged(src, c0), query_dst(slot))):
                copy = pltpu.make_async_remote_copy(
                    a, b, stage_send.at[t, src, c0], recv.at[t, slot],
                    device_id=(row, src), device_id_type=MESH)
                if act == "start":
                    pltpu.make_async_copy(a, a, stage_recv.at[t, src, c0]).wait()
                    copy.start()
                else:
                    copy.wait_send()

    def key_send(i, act):
        h = (s + i) % heads
        cols = pl.ds(pl.multiple_of(h * HEAD_DIM, HEAD_DIM), HEAD_DIM)
        for t, (a, b) in enumerate(((k_ref, ko), (v_ref, vo))):
            if i == 0:
                if act == "start":
                    pltpu.make_async_copy(a.at[:, cols], b.at[row], kv_recv.at[t, s]).start()
            else:
                there = pltpu.make_async_remote_copy(
                    a.at[:, cols], b.at[row], kv_send.at[t, i], kv_recv.at[t, s],
                    device_id=(h * 2 + core, z), device_id_type=MESH)
                there.start() if act == "start" else there.wait_send()

    def arrived(j):
        for t, b in enumerate(query_dst(j)):
            pltpu.make_async_copy(b, b, recv.at[t, j]).wait()

    def key_forward(i, act):
        src = (s + heads - i) % heads
        for t, b in enumerate((ko, vo)):
            at = b.at[src * 2 + core]
            copy = pltpu.make_async_remote_copy(
                at, at, fwd_send.at[t, src], fwd_recv.at[t, src],
                device_id=(partner, z), device_id_type=MESH)
            if act == "start":
                pltpu.make_async_copy(at, at, kv_recv.at[t, src]).wait()
                copy.start()
            else:
                copy.wait_send()
                got = b.at[src * 2 + 1 - core]
                pltpu.make_async_copy(got, got, fwd_recv.at[t, src]).wait()

    for i in range(heads):
        for half in range(2):
            query_send(i, half, "start")
    for i in range(heads):
        key_send(i, "start")
    for i in range(heads):
        for c0 in range(2):
            stage_forward(i, c0, "start")
    for i in range(heads):
        key_forward(i, "start")
    for j in range(2 * planes):
        arrived(j)
    for i in range(heads):
        for half in range(2):
            query_send(i, half, "wait")
        key_send(i, "wait")
        key_forward(i, "wait")
        for c0 in range(2):
            stage_forward(i, c0, "wait")


def spread(planes, q, g, nd, k, v):
    n = q.shape[0]
    slots = 2 * planes
    anywhere = pl.BlockSpec(memory_space=pl.ANY)
    whole = pl.BlockSpec(memory_space=pltpu.VMEM)
    dma = pltpu.SemaphoreType.DMA
    tiles = jax.ShapeDtypeStruct((slots, n // 2, HEAD_DIM), jnp.bfloat16)
    keys = jax.ShapeDtypeStruct((2 * KV_HEADS, n, HEAD_DIM), jnp.bfloat16)
    stage = pltpu.VMEM((KV_HEADS, 2, n // 2, HEAD_DIM), jnp.bfloat16)
    return pl.pallas_call(
        functools.partial(spread_kernel, planes),
        out_shape=(tiles, tiles, jax.ShapeDtypeStruct((slots, 2, n // 2), jnp.float32), keys, keys),
        in_specs=[anywhere] * 5,
        out_specs=(whole,) * 5,
        scratch_shapes=[
            stage, stage, pltpu.VMEM((KV_HEADS, 2, 2, n // 2), jnp.float32),
            dma((3, KV_HEADS, 2)), dma((3, slots)),
            dma((3, KV_HEADS, 2)), dma((3, KV_HEADS, 2)),
            dma((2, KV_HEADS)), dma((2, KV_HEADS)), dma((2, KV_HEADS)), dma((2, KV_HEADS)),
        ],
        compiler_params=pltpu.CompilerParams(
            has_side_effects=True, vmem_limit_bytes=28 * 1024 * 1024),
        name="spread",
    )(q, g, nd, k, v)


def attention_kernel(
    which, docs, ends_ref, q_ref, g_ref, nd_ref, k_ref, v_ref, *refs,
):
    before, (dq_ref, dk_ref, dv_ref, dq_acc, dk_acc, dv_acc) = refs[:-6], refs[-6:]
    slots, tile_q = q_ref.shape[0], q_ref.shape[1]
    segment = dk_acc.shape[0]
    tile_k = dk_tile = min(TILE_K, segment)
    core = lax.axis_index("qrow") % 2
    base = lax.axis_index("kcol") * segment

    def doc_start(position):
        start = jnp.zeros_like(position)
        for d in range(docs):
            start = jnp.where(position >= ends_ref[d], ends_ref[d], start)
        return start

    for i, acc in enumerate((dk_acc, dv_acc)):
        acc[...] = before[i][...].astype(jnp.float32) if before else jnp.zeros_like(acc)

    def query_step(j, carry):
        q_lo = which * segment + (2 * j + (core + j) % 2) * tile_q
        q_pos = q_lo + lax.broadcasted_iota(jnp.int32, (1, tile_q), 1)
        q_start = doc_start(q_pos + base) - base
        lo = jnp.maximum(doc_start(q_lo + base) - base, 0)
        hi = jnp.minimum(q_lo + tile_q, segment)
        last_start = jnp.maximum(doc_start(q_lo + base + tile_q - 1) - base, 0)
        first = lo // tile_k
        last = (hi + tile_k - 1) // tile_k
        full_lo = jnp.minimum((last_start + tile_k - 1) // tile_k, last)
        full_hi = jnp.maximum(jnp.minimum((q_lo + 1) // tile_k, last), full_lo)
        q = q_ref[j]
        g = g_ref[j]
        nd = nd_ref[j]
        norm = nd[0:1, :]
        delta = nd[1:2, :]
        dq_acc[...] = jnp.zeros_like(dq_acc)

        def key_step(masked, kt, carry):
            rows = pl.ds(pl.multiple_of(kt * tile_k, tile_k), tile_k)
            k = k_ref[rows, :]
            v = v_ref[rows, :]
            s = dot(k, q, ((1,), (1,)))
            dp = dot(v, g, ((1,), (1,)))
            p = jnp.exp2(s * (SCALING * LOG2E) - norm)
            if masked:
                k_pos = kt * tile_k + lax.broadcasted_iota(jnp.int32, (tile_k, 1), 0)
                p = jnp.where((k_pos <= q_pos) & (k_pos >= q_start), p, 0.0)
            ds = (p * (dp - delta)).astype(jnp.bfloat16)
            dv_acc[rows, :] += dot(p.astype(jnp.bfloat16), g, ((1,), (0,)))
            dk_acc[rows, :] += dot(ds, q, ((1,), (0,)))
            dq_acc[...] += dot(k, ds, ((0,), (0,)))
            return carry

        @pl.when(lo < hi)
        def _():
            lax.fori_loop(first, full_lo, functools.partial(key_step, True), 0)
            lax.fori_loop(full_lo, full_hi, functools.partial(key_step, False), 0)
            lax.fori_loop(full_hi, last, functools.partial(key_step, True), 0)

        dq_ref[j] = (dq_acc[...] * SCALING).T.astype(jnp.bfloat16)
        return carry

    lax.fori_loop(0, slots, query_step, 0)

    def finish(kt, carry):
        rows = pl.ds(pl.multiple_of(kt * tile_k, tile_k), tile_k)
        dk_ref[rows, :] = (dk_acc[rows, :] * (SCALING if before else 1.0)).astype(jnp.bfloat16)
        dv_ref[rows, :] = dv_acc[rows, :].astype(jnp.bfloat16)
        return carry

    lax.fori_loop(0, segment // tile_k, finish, 0)


def attention(which, ends, q, g, nd, k, v, *before):
    slots, tile_q = q.shape[:2]
    segment = k.shape[0]
    whole = pl.BlockSpec(memory_space=pltpu.VMEM)
    scalars = pl.BlockSpec(memory_space=pltpu.SMEM)
    return pl.pallas_call(
        functools.partial(attention_kernel, which, ends.shape[0]),
        out_shape=(
            jax.ShapeDtypeStruct(q.shape, jnp.bfloat16),
            jax.ShapeDtypeStruct(k.shape, jnp.bfloat16),
            jax.ShapeDtypeStruct(v.shape, jnp.bfloat16),
        ),
        in_specs=[scalars] + [whole] * (5 + len(before)),
        out_specs=(whole,) * 3,
        scratch_shapes=[
            pltpu.VMEM((HEAD_DIM, tile_q), jnp.float32),
            pltpu.VMEM((segment, HEAD_DIM), jnp.float32),
            pltpu.VMEM((segment, HEAD_DIM), jnp.float32),
        ],
        compiler_params=pltpu.CompilerParams(vmem_limit_bytes=36 * 1024 * 1024),
        cost_estimate=pl.CostEstimate(
            flops=5 * slots * tile_q * segment * HEAD_DIM, bytes_accessed=0, transcendentals=0),
        name=("attention_own", "attention_next")[which],
    )(ends, q, g, nd, k, v, *before)


def collect_kernel(
    planes, dq_own, dq_next, dk_ref, dv_ref, dqo, dko, dvo, parts, pair, summed,
    send, recv, pair_send, pair_recv, kv_send, kv_recv,
):
    row = lax.axis_index("qrow")
    z = lax.axis_index("kcol")
    s = row // 2
    core = row % 2
    heads = KV_HEADS
    tile = dq_own.shape[1]
    n = dko.shape[0]
    partner = s * 2 + 1 - core
    mine = pl.ds(pl.multiple_of(s * HEAD_DIM, HEAD_DIM), HEAD_DIM)
    kv = ((dk_ref, dko), (dv_ref, dvo))

    def trade(i, act):
        to = (s + 1 + i) % heads
        for t, (a, _) in enumerate(kv):
            copy = pltpu.make_async_remote_copy(
                a.at[to * 2 + 1 - core], pair.at[t, to], pair_send.at[t, to], pair_recv.at[t, to],
                device_id=(partner, z), device_id_type=MESH)
            copy.start() if act == "start" else copy.wait_send()

    def query_return(which, c0, z0, act):
        j = c0 * planes + z0
        half = (core + z0) % 2
        dq_ref = (dq_own, dq_next)[which]
        to = (z + which) * 2 + c0
        home = (to == row) & (z0 == z)
        copy = pltpu.make_async_remote_copy(
            dq_ref.at[j], parts.at[which, s, half],
            send.at[which, j], recv.at[which, s, half],
            device_id=(to, z0), device_id_type=MESH)

        def move():
            if act == "start":
                @pl.when(home)
                def _():
                    parts[which, s, half] = dq_ref[j]
                pl.when(jnp.logical_not(home))(copy.start)
            else:
                pl.when(jnp.logical_not(home))(copy.wait_send)
        if which == 0:
            move()
        else:
            pl.when(z + 1 < planes)(move)

    def every_query(act):
        for d in sorted(range(planes), key=lambda d: (d == 0, abs(2 * d - planes))):
            for c0 in range(2):
                for which in range(2):
                    query_return(which, c0, (z + d) % planes, act)

    for i in range(heads):
        trade(i, "start")
    every_query("start")

    def key_return(i, act):
        to = (s + 1 + i) % heads
        if i == heads - 1 and act != "sum":
            return
        for t, (a, out) in enumerate(kv):
            if act == "sum":
                got = pair.at[t, to]
                pltpu.make_async_copy(got, got, pair_recv.at[t, to]).wait()
                total = (a[to * 2 + core].astype(jnp.float32)
                         + pair[t, to].astype(jnp.float32)).astype(jnp.bfloat16)
                if i == heads - 1:
                    out[:, mine] = total
                else:
                    summed[t, to] = total
            else:
                copy = pltpu.make_async_remote_copy(
                    summed.at[t, to], out.at[:, mine], kv_send.at[t, to], kv_recv.at[t, s],
                    device_id=(to * 2 + core, z), device_id_type=MESH)
                copy.start() if act == "start" else copy.wait_send()

    for i in range(heads):
        key_return(i, "sum")
        if i:
            key_return(i - 1, "start")

    def add_up(h, half):
        home = (h == s) & (z == s) & (half == (core + z) % 2)
        home_next = (h == s) & (s == z + 1) & (half == (core + z) % 2)
        got = parts.at[0, h, half]
        pl.when(jnp.logical_not(home))(pltpu.make_async_copy(got, got, recv.at[0, h, half]).wait)
        rows = pl.ds(half * tile, tile)
        cols = pl.ds(h * HEAD_DIM, HEAD_DIM)

        @pl.when(s == 0)
        def _():
            dqo[rows, cols] = parts[0, h, half]

        @pl.when(s > 0)
        def _():
            more = parts.at[1, h, half]
            pl.when(jnp.logical_not(home_next))(
                pltpu.make_async_copy(more, more, recv.at[1, h, half]).wait)
            dqo[rows, cols] = (parts[0, h, half].astype(jnp.float32)
                               + parts[1, h, half].astype(jnp.float32)).astype(jnp.bfloat16)

    for h in range(heads):
        for half in range(2):
            add_up(h, half)
    for i in range(heads):
        trade(i, "wait")
        key_return(i, "wait")
    every_query("wait")
    for i in range(heads - 1):
        src = (s + 1 + i) % heads
        cols = pl.ds(pl.multiple_of(src * HEAD_DIM, HEAD_DIM), HEAD_DIM)
        for t, (_, out) in enumerate(kv):
            got = out.at[:, cols]
            pltpu.make_async_copy(got, got, kv_recv.at[t, src]).wait()


def collect(planes, dq, dq_next, dk, dv):
    tile = dq.shape[1]
    n = dk.shape[1]
    whole = pl.BlockSpec(memory_space=pltpu.VMEM)
    dma = pltpu.SemaphoreType.DMA
    out = jax.ShapeDtypeStruct((n, KV_HEADS * HEAD_DIM), jnp.bfloat16)
    return pl.pallas_call(
        functools.partial(collect_kernel, planes),
        out_shape=(out,) * 3,
        in_specs=[whole] * 4,
        out_specs=(whole,) * 3,
        scratch_shapes=[
            pltpu.VMEM((2, KV_HEADS, 2, tile, HEAD_DIM), jnp.bfloat16),
            pltpu.VMEM((2, KV_HEADS, n, HEAD_DIM), jnp.bfloat16),
            pltpu.VMEM((2, KV_HEADS, n, HEAD_DIM), jnp.bfloat16),
            dma((2, 2 * planes)), dma((2, KV_HEADS, 2)),
            dma((2, KV_HEADS)), dma((2, KV_HEADS)), dma((2, KV_HEADS)), dma((2, KV_HEADS)),
        ],
        compiler_params=pltpu.CompilerParams(
            has_side_effects=True, vmem_limit_bytes=28 * 1024 * 1024),
        name="collect",
    )(dq, dq_next, dk, dv)


def by_segment(planes, query_states, key_states, value_states, saved_output, output_grad,
               normalizer, doc_lengths):
    n = query_states.shape[0]
    product = output_grad.astype(jnp.float32) * saved_output.astype(jnp.float32)
    member = jnp.repeat(jnp.eye(KV_HEADS, dtype=jnp.float32), HEAD_DIM, axis=1)
    row_delta = lax.dot_general(
        member, product, (((1,), (1,)), ((), ())), precision=lax.Precision.HIGHEST)
    nd = jnp.stack([(normalizer * LOG2E).T, row_delta], axis=1)
    nd = nd.reshape(KV_HEADS, 2, 2, n // 2).transpose(0, 2, 1, 3)
    q, g, nd, k, v = spread(planes, query_states, output_grad, nd, key_states, value_states)
    ends = jnp.cumsum(doc_lengths)
    k, v = k.reshape(-1, HEAD_DIM), v.reshape(-1, HEAD_DIM)
    down = [(i + 1, i) for i in range(planes - 1)]
    shifted = [lax.ppermute(x, "kcol", down) for x in (q, g, nd)]
    dq, dk, dv = attention(0, ends, q, g, nd, k, v)
    dq_next, dk, dv = attention(1, ends, *shifted, k, v, dk, dv)
    return collect(planes, dq, dq_next, dk.reshape(-1, n, HEAD_DIM), dv.reshape(-1, n, HEAD_DIM))


DEAL_Q = 512
DEAL_K = 256
Q_AXES = ("yx", "core", "ko", "head")
K_AXES = ("ko", "head", "yx", "core")


def dealt_kernel(
    piece, groups, docs, ends_ref, where_ref, q_ref, g_ref, nd_ref, k_ref, v_ref,
    dq_ref, dk_ref, dv_ref, dq_acc, dk_acc, dv_acc,
):
    tile_q = nd_ref.shape[2]
    tile_k = dk_acc.shape[0]
    q_tiles = q_ref.shape[0] // tile_q
    k_tiles = k_ref.shape[0] // tile_k
    core = where_ref[0]
    group = where_ref[1]
    run = 2 * piece

    def key_token(i):
        return (i // run) * (groups * run) + group * run + i % run

    def doc_end(position):
        end = jnp.zeros_like(position)
        for d in range(docs - 1, -1, -1):
            end = jnp.where(position < ends_ref[d], ends_ref[d], end)
        return end

    dq_acc[...] = jnp.zeros_like(dq_acc)
    q_local = lax.broadcasted_iota(jnp.int32, (1, tile_q), 1)
    q_base = (q_local // piece) * run + core * piece + q_local % piece

    def key_step(kt, carry):
        k_lo = kt * tile_k
        rows = pl.ds(pl.multiple_of(k_lo, tile_k), tile_k)
        k = k_ref[rows, :]
        v = v_ref[rows, :]
        k_t = k.T
        k_pos = key_token(k_lo + lax.broadcasted_iota(jnp.int32, (tile_k, 1), 0))
        k_end = doc_end(k_pos)
        first = key_token(k_lo) // (2 * tile_q)
        last = (doc_end(key_token(k_lo + tile_k - 1)) - 1) // (2 * tile_q)
        dk_acc[...] = jnp.zeros_like(dk_acc)
        dv_acc[...] = jnp.zeros_like(dv_acc)

        def query_step(qt, carry):
            q_rows = pl.ds(pl.multiple_of(qt * tile_q, tile_q), tile_q)
            q = q_ref[q_rows, :]
            g = g_ref[q_rows, :]
            nd = nd_ref[qt]
            norm = nd[0:1, :]
            delta = nd[1:2, :]
            q_pos = q_base + qt * (2 * tile_q)
            s = dot(k, q, ((1,), (1,)))
            dp = dot(v, g, ((1,), (1,)))
            allowed = (k_pos <= q_pos) & (q_pos < k_end)
            p = jnp.where(allowed, jnp.exp2(s * (SCALING * LOG2E) - norm), 0.0)
            ds = (p * (dp - delta)).astype(jnp.bfloat16)
            dv_acc[...] += dot(p.astype(jnp.bfloat16), g, ((1,), (0,)))
            dk_acc[...] += dot(ds, q, ((1,), (0,)))
            dq_acc[qt] += dot(k_t, ds, ((1,), (0,)))
            return carry

        lax.fori_loop(first, last + 1, query_step, 0)
        dk_ref[rows, :] = (dk_acc[...] * SCALING).astype(jnp.bfloat16)
        dv_ref[rows, :] = dv_acc[...].astype(jnp.bfloat16)
        return carry

    lax.fori_loop(0, k_tiles, key_step, 0)

    def finish(qt, carry):
        q_rows = pl.ds(pl.multiple_of(qt * tile_q, tile_q), tile_q)
        dq_ref[q_rows, :] = (dq_acc[qt] * SCALING).T.astype(jnp.bfloat16)
        return carry

    lax.fori_loop(0, q_tiles, finish, 0)


def dealt_attention(piece, groups, ends, place, q, g, nd, k, v):
    tile_q = nd.shape[2]
    tile_k = min(DEAL_K, k.shape[0])
    whole = pl.BlockSpec(memory_space=pltpu.VMEM)
    scalars = pl.BlockSpec(memory_space=pltpu.SMEM)
    return pl.pallas_call(
        functools.partial(dealt_kernel, piece, groups, ends.shape[0]),
        out_shape=(
            jax.ShapeDtypeStruct(q.shape, jnp.bfloat16),
            jax.ShapeDtypeStruct(k.shape, jnp.bfloat16),
            jax.ShapeDtypeStruct(v.shape, jnp.bfloat16),
        ),
        in_specs=[scalars, scalars, whole, whole, whole, whole, whole],
        out_specs=(whole, whole, whole),
        scratch_shapes=[
            pltpu.VMEM((q.shape[0] // tile_q, HEAD_DIM, tile_q), jnp.float32),
            pltpu.VMEM((tile_k, HEAD_DIM), jnp.float32),
            pltpu.VMEM((tile_k, HEAD_DIM), jnp.float32),
        ],
        compiler_params=pltpu.CompilerParams(vmem_limit_bytes=58 * 1024 * 1024),
    )(ends, place, q, g, nd, k, v)


def per_device(sizes, query_states, key_states, value_states, saved_output, output_grad,
               normalizer, doc_lengths):
    yx, core, ko, head = (sizes[a] for a in Q_AXES)
    devices = yx * core * ko * head
    rows = query_states.shape[0]
    piece = rows // (yx * ko * core)
    groups = yx * ko
    row_delta = jnp.sum(
        (output_grad.astype(jnp.float32) * saved_output.astype(jnp.float32)).reshape(
            rows, KV_HEADS, HEAD_DIM
        ),
        axis=2,
    )

    def deal(x, key_side):
        x = x.reshape(yx, ko, core, piece, KV_HEADS, -1)
        order = (1, 4, 0, 2, 3, 5) if key_side else (0, 2, 1, 4, 3, 5)
        x = x.transpose(order).reshape(devices, piece, x.shape[-1])
        return lax.all_to_all(x, K_AXES if key_side else Q_AXES, 0, 0, tiled=True)

    def undeal(x, key_side):
        x = lax.all_to_all(x, K_AXES if key_side else Q_AXES, 0, 0, tiled=True)
        if key_side:
            x = x.reshape(ko, head, yx, core, piece, HEAD_DIM).transpose(2, 0, 3, 4, 1, 5)
        else:
            x = x.reshape(yx, core, ko, head, piece, HEAD_DIM).transpose(0, 2, 1, 4, 3, 5)
        return x.reshape(rows, KV_HEADS * HEAD_DIM)

    nd = jnp.stack([normalizer * LOG2E, row_delta], axis=-1)
    nd = deal(nd, False)
    q = deal(query_states, False)
    g = deal(output_grad, False)
    k = deal(key_states, True)
    v = deal(value_states, True)

    def gather(x, axes):
        x = lax.all_gather(x, axes, axis=0, tiled=False)
        return x.transpose(1, 0, 2, 3).reshape(-1, x.shape[-1])

    nd = gather(nd, ("yx", "ko"))
    q = gather(q, ("yx", "ko"))
    g = gather(g, ("yx", "ko"))
    k = gather(k, ("core",))
    v = gather(v, ("core",))
    tile_q = min(DEAL_Q, q.shape[0])
    nd = nd.reshape(-1, tile_q, 2).transpose(0, 2, 1)
    place = jnp.stack(
        [lax.axis_index("core"), lax.axis_index("yx") * ko + lax.axis_index("ko")]
    ).astype(jnp.int32)
    ends = jnp.cumsum(doc_lengths)
    dq, dk, dv = dealt_attention(piece, groups, ends, place, q, g, nd, k, v)

    def total(x, parts, axes):
        x = x.reshape(devices, parts, piece, HEAD_DIM).transpose(1, 0, 2, 3)
        x = lax.all_to_all(x, axes, 0, 0, tiled=True)
        return jnp.sum(x.astype(jnp.float32), axis=0).astype(jnp.bfloat16)

    dq = undeal(total(dq, groups, ("yx", "ko")), False)
    dk = undeal(total(dk, core, ("core",)), True)
    dv = undeal(total(dv, core, ("core",)), True)
    return dq, dk, dv


def solution(mesh):
    qrow = mesh.shape["qrow"]
    kcol = mesh.shape["kcol"]

    def whole(*args):
        tokens = args[0].shape[0]
        if qrow == 2 * KV_HEADS and kcol == KV_HEADS and tokens // kcol >= MOST:
            by_query, by_key = P(("qrow", "kcol"), None), P(("kcol", "qrow"), None)
            place, body = mesh, functools.partial(by_segment, kcol)
        else:
            sizes = {"yx": qrow // 2, "core": 2, "ko": kcol // KV_HEADS, "head": KV_HEADS}
            place = Mesh(mesh.devices.reshape([sizes[a] for a in Q_AXES]), Q_AXES)
            by_query, by_key = P(Q_AXES, None), P(K_AXES, None)
            body = functools.partial(per_device, sizes)
        return jax.shard_map(
            body,
            mesh=place,
            in_specs=(by_query, by_key, by_key, by_query, by_query, by_query, P()),
            out_specs=(by_query, by_key, by_key),
            check_vma=False,
        )(*args)

    return whole
```
